32 devices in a mesh: req: 2 (over y), blk: 4 (over z), uly: 4 (over x, core).
Axes of the slice: x: 2, y: 2, z: 4, core: 2. Of those that a mesh axis runs over, the one named last changes fastest.
Arguments:
- video_qkv: bfloat16 [3, 2048, 3072], P(None, ('req', 'blk', 'uly')), parts along dimension 1, may hold values from -16 to 16
- text_qkv: bfloat16 [3, 64, 3072], P(None, ('req', 'blk', 'uly')), parts along dimension 1, may hold values from -9.5625 to 9.5625
- video_gate: float32 [6144], P('req'), parts along dimension 0, may hold values from 1 to 4
- text_gate: float32 [6144], P('req'), parts along dimension 0, may hold values from 1 to 4
Outputs:
- video_out: bfloat16 [2048, 3072], P(('req', 'blk', 'uly')), parts along dimension 0
- text_out: bfloat16 [64, 3072], P(('req', 'blk', 'uly')), parts along dimension 0
The draws below stay inside these ranges and needn't reach their ends.
There are 2 independent parts, one for each index of `req`. The reference program is written for one: setup_inputs(seed, part) draws one part's arguments, and reference() takes and returns one part's arrays. A program takes and returns all parts, laid end to end along the dimension named above; each array names one. Nothing has to cross between parts.
All inputs are finite; a program needn't handle non-finite values.
Results may differ from the reference program's by a relative error of at most 0.0085.
Values may be sent and summed in bfloat16 or wider, within the bound.
No kernel may reach another device: no remote copies, remote signals or barrier semaphores. Data moves between devices by JAX's collectives and lax.ppermute only.
A program may use at most 128 MiB of HBM per device.

```python
import math
import jax
import jax.numpy as jnp
from jax import lax

HEADS = 24
HD = 128
D = 3072
TOKENS = 1024
TXT = 32


def draw_video_qkv(key, part):
    base = jnp.clip(jax.random.normal(key, (3, TOKENS, D), jnp.float32) * 1.6, -9.6, 9.6)
    return base.astype(jnp.bfloat16)


def level_of(own_key, shape, cuts, least, largest):
    level, own = 1.0, jax.random.fold_in(own_key, 6)
    for dim, parts in cuts:
        steps = jnp.exp(jax.random.uniform(jax.random.fold_in(own, dim), (parts,), jnp.float32, least / len(cuts), largest / len(cuts)))
        level = level * jnp.repeat(steps, shape[dim] // parts).reshape([-1 if axis == dim else 1 for axis in range(len(shape))])
    return level


def bell_draw(stream_key, dims, scale, bound, shards=(), dtype=jnp.bfloat16):
    factor_of = level_of(stream_key, dims, shards, -0.22, 0.18) if shards else 1.0
    entries = jax.random.normal(stream_key, dims, jnp.float32) * scale * factor_of
    return jnp.minimum(jnp.maximum(entries, -bound), bound).astype(dtype)


def setup_inputs(seed: int = 0, part: int = 0) -> dict:
    splits = jax.random.split(jax.random.key(seed), 5)
    part_splits = jax.random.split(jax.random.fold_in(splits[4], part), 5)
    return {
        "video_qkv": draw_video_qkv(jax.random.fold_in(jax.random.fold_in(splits[4], part), 71), part),
        "text_qkv": bell_draw(part_splits[1], (3, TXT, D), 1.6, 9.5625, ((1, 16),)),
        "video_gate": jnp.clip(jnp.exp(jax.random.uniform(part_splits[2], (D,), jnp.float32, math.log(1.0), math.log(4.0))), 1.0, 4.0),
        "text_gate": jnp.clip(jnp.exp(jax.random.uniform(part_splits[3], (D,), jnp.float32, math.log(1.0), math.log(4.0))), 1.0, 4.0),
    }


def one_head(operands):
    queries, keys, values = operands
    scores = jnp.dot(queries, keys.T, precision=lax.Precision.HIGHEST) / math.sqrt(HD)
    best = lax.optimization_barrier(jnp.max(scores, axis=1))
    raised = jnp.exp(scores - best[:, None])
    total = lax.optimization_barrier(jnp.sum(raised, axis=1))
    weights = lax.optimization_barrier(raised.astype(jnp.bfloat16)).astype(jnp.float32)
    return jnp.dot(weights, values, precision=lax.Precision.HIGHEST) / total[:, None]

def reference(video_qkv, text_qkv, video_gate, text_gate):
    joint = jnp.concatenate((video_qkv, text_qkv), axis=1).astype(jnp.float32)
    length = joint.shape[1]
    split = joint.reshape(3, length, HEADS, HD).transpose(0, 2, 1, 3)
    heads_out = lax.map(one_head, (split[0], split[1], split[2]))
    attended = heads_out.transpose(1, 0, 2).reshape(length, HEADS * HD).astype(jnp.bfloat16)
    attended = lax.optimization_barrier(attended).astype(jnp.float32)
    video_out = (attended[:TOKENS] * video_gate[None, :]).astype(jnp.bfloat16)
    text_out = (attended[TOKENS:] * text_gate[None, :]).astype(jnp.bfloat16)
    return (video_out, text_out)
```

```python
import functools
import math

import jax
import jax.numpy as jnp
from jax import lax
from jax.experimental import pallas as pl
from jax.experimental.pallas import tpu as pltpu
from jax.sharding import Mesh, PartitionSpec as P

HEADS = 24
HD = 128
VMEM = pltpu.VMEM
ROW_TILE = 8


def up(n, m):
    return -(-n // m) * m


def vspec():
    return pl.BlockSpec(memory_space=VMEM)


def pack_kernel(groups, copies, video, text, q_out, kv_out):
    rows, trows = video.shape[1], text.shape[1]
    width = q_out.shape[2]
    q_pad = q_out.shape[1] - rows - trows
    kv_pad = kv_out.shape[2] - 2 * rows - 2 * trows
    for g in range(groups):
        lanes = slice(g * width, (g + 1) * width)
        q_out[g, :rows, :] = video[0, :, lanes]
        parts = [text[0, :, lanes].astype(jnp.float32), jnp.zeros((q_pad, width), jnp.float32)]
        q_out[g, rows:, :] = jnp.concatenate(parts, axis=0).astype(jnp.bfloat16)
        parts = [
            text[1, :, lanes].astype(jnp.float32),
            text[2, :, lanes].astype(jnp.float32),
            jnp.zeros((kv_pad, width), jnp.float32),
        ]
        tail = jnp.concatenate(parts, axis=0).astype(jnp.bfloat16)
        for c in range(copies):
            kv_out[c, g, :rows, :] = video[1, :, lanes]
            kv_out[c, g, rows : 2 * rows, :] = video[2, :, lanes]
            kv_out[c, g, 2 * rows :, :] = tail


def select_rows(count, tile, first, trows):
    i = lax.broadcasted_iota(jnp.int32, (count * trows, count * tile), 0)
    j = lax.broadcasted_iota(jnp.int32, (count * trows, count * tile), 1)
    want = (i // trows) * tile + first + i % trows
    return jnp.where(j == want, 1.0, 0.0).astype(jnp.bfloat16)


def attend_kernel(rows, trows, per, q_in, kv_in, out):
    sources, qrows, width = q_in.shape
    count, kvrows, _ = kv_in.shape
    heads = width // HD
    total_q = sources * qrows
    tile = kvrows - 2 * rows
    scale = math.log2(math.e) / math.sqrt(HD)
    pick_k = select_rows(per, tile, 0, trows)
    pick_v = select_rows(per, tile, trows, trows)
    nt = (((1,), (1,)), ((), ()))

    def block(h, start):
        lanes = slice(h * HD, (h + 1) * HD)
        span = pl.ds(start, per)
        k = kv_in[span, :rows, lanes].reshape(per * rows, HD)
        v = kv_in[span, rows : 2 * rows, lanes].reshape(per * rows, HD)
        t = kv_in[span, 2 * rows :, lanes].reshape(per * tile, HD)
        kt = jnp.dot(pick_k, t, preferred_element_type=jnp.float32).astype(jnp.bfloat16)
        vt = jnp.dot(pick_v, t, preferred_element_type=jnp.float32).astype(jnp.bfloat16)
        return k, v, kt, vt

    def scores(q, k):
        return lax.dot_general(q, k, nt, preferred_element_type=jnp.float32)

    def weigh(s, best):
        return jnp.exp2((s - best) * scale).astype(jnp.bfloat16)

    def with_ones(v):
        return jnp.concatenate([v, jnp.ones_like(v)], axis=1)

    for h in range(heads):
        lanes = slice(h * HD, (h + 1) * HD)
        q = q_in[:, :, lanes].reshape(total_q, HD)

        def step(i, state):
            k, v, kt, vt = block(h, i * per)
            s, st = scores(q, k), scores(q, kt)
            best = jnp.maximum(jnp.max(s, axis=1, keepdims=True), jnp.max(st, axis=1, keepdims=True))
            if state is not None:
                best = jnp.maximum(best, state[0])
            new = jnp.dot(weigh(s, best), with_ones(v), preferred_element_type=jnp.float32)
            new += jnp.dot(weigh(st, best), with_ones(vt), preferred_element_type=jnp.float32)
            if state is not None:
                new += state[1] * jnp.exp2((state[0] - best) * scale)
            return best, new

        state = step(0, None)
        if count > per:
            state = lax.fori_loop(1, count // per, step, state)
        summed = state[1]
        o = summed[:, :HD] / summed[:, HD:]
        out[:, :, lanes] = o.reshape(sources, qrows, HD).astype(jnp.bfloat16)


def unpack_kernel(o_in, video_gate, text_gate, video_out, text_out):
    rows, trows = video_out.shape[0], text_out.shape[0]
    groups, _, width = o_in.shape
    for g in range(groups):
        lanes = slice(g * width, (g + 1) * width)
        x = o_in[g, :rows, :].astype(jnp.float32)
        video_out[:, lanes] = (x * video_gate[:, lanes]).astype(jnp.bfloat16)
        x = o_in[g, rows:, :].astype(jnp.float32)[:trows]
        text_out[:, lanes] = (x * text_gate[:, lanes]).astype(jnp.bfloat16)


def on_device(video_qkv, text_qkv, video_gate, text_gate):
    halves, planes, uly = lax.axis_size("half"), lax.axis_size("plane"), lax.axis_size("uly")
    groups = planes * uly
    count = halves * groups
    rows, trows = video_qkv.shape[1], text_qkv.shape[1]
    width = HEADS // groups * HD
    q_rows = up(rows + trows, ROW_TILE)
    kv_rows = up(2 * rows + 2 * trows, ROW_TILE)
    bf16 = jnp.bfloat16
    limit = pltpu.CompilerParams(vmem_limit_bytes=56 * 1024 * 1024)
    q_pack, kv_pack = pl.pallas_call(
        functools.partial(pack_kernel, groups, halves),
        out_shape=(
            jax.ShapeDtypeStruct((groups, q_rows, width), bf16),
            jax.ShapeDtypeStruct((halves, groups, kv_rows, width), bf16),
        ),
        in_specs=[vspec()] * 2,
        out_specs=(vspec(), vspec()),
        name="pack",
    )(video_qkv, text_qkv)
    kv = lax.all_to_all(
        kv_pack.reshape(count, kv_rows, width),
        ("half", "plane", "uly"), split_axis=0, concat_axis=0, tiled=True,
    )
    q = lax.all_to_all(q_pack, ("plane", "uly"), split_axis=0, concat_axis=0, tiled=True)
    per = count
    while per * rows > 1024 and per % 2 == 0:
        per //= 2
    o = pl.pallas_call(
        functools.partial(attend_kernel, rows, trows, per),
        out_shape=jax.ShapeDtypeStruct((groups, q_rows, width), bf16),
        in_specs=[vspec()] * 2,
        out_specs=vspec(),
        compiler_params=limit,
        name="attend",
    )(q, kv)
    back = lax.all_to_all(o, ("plane", "uly"), split_axis=0, concat_axis=0, tiled=True)
    return pl.pallas_call(
        unpack_kernel,
        out_shape=(
            jax.ShapeDtypeStruct((rows, HEADS * HD), bf16),
            jax.ShapeDtypeStruct((trows, HEADS * HD), bf16),
        ),
        in_specs=[vspec()] * 3,
        out_specs=(vspec(), vspec()),
        name="unpack",
    )(back, video_gate[None, :], text_gate[None, :])


def solution(mesh):
    req, blk, uly = (mesh.shape[name] for name in ("req", "blk", "uly"))
    planes = max(p for p in range(1, blk + 1) if blk % p == 0 and HEADS % (p * uly) == 0)
    fine = Mesh(
        mesh.devices.reshape(req, blk // planes, planes, uly), ("req", "half", "plane", "uly")
    )
    every = ("req", "half", "plane", "uly")
    in_specs = (P(None, every, None), P(None, every, None), P("req"), P("req"))
    out_specs = (P(every, None), P(every, None))
    return jax.shard_map(
        on_device, mesh=fine, in_specs=in_specs, out_specs=out_specs, check_vma=False
    )
```

```python
import functools
import math

import jax
import jax.numpy as jnp
from jax import lax
from jax.experimental import pallas as pl
from jax.experimental.pallas import tpu as pltpu
from jax.sharding import Mesh, PartitionSpec as P

HEADS = 24
HD = 128
VMEM = pltpu.VMEM
ROW_TILE = 8


def up(n, m):
    return -(-n // m) * m


def vspec():
    return pl.BlockSpec(memory_space=VMEM)


def pack_kernel(groups, copies, video, text, q_out, kv_out):
    rows, trows = video.shape[1], text.shape[1]
    width = q_out.shape[2]
    q_pad = q_out.shape[1] - rows - trows
    kv_pad = kv_out.shape[2] - 2 * rows - 2 * trows
    for g in range(groups):
        lanes = slice(g * width, (g + 1) * width)
        q_out[g, :rows, :] = video[0, :, lanes]
        parts = [text[0, :, lanes].astype(jnp.float32), jnp.zeros((q_pad, width), jnp.float32)]
        q_out[g, rows:, :] = jnp.concatenate(parts, axis=0).astype(jnp.bfloat16)
        parts = [
            text[1, :, lanes].astype(jnp.float32),
            text[2, :, lanes].astype(jnp.float32),
            jnp.zeros((kv_pad, width), jnp.float32),
        ]
        tail = jnp.concatenate(parts, axis=0).astype(jnp.bfloat16)
        for c in range(copies):
            kv_out[c, g, :rows, :] = video[1, :, lanes]
            kv_out[c, g, rows : 2 * rows, :] = video[2, :, lanes]
            kv_out[c, g, 2 * rows :, :] = tail


def select_rows(count, tile, first, trows):
    i = lax.broadcasted_iota(jnp.int32, (count * trows, count * tile), 0)
    j = lax.broadcasted_iota(jnp.int32, (count * trows, count * tile), 1)
    want = (i // trows) * tile + first + i % trows
    return jnp.where(j == want, 1.0, 0.0).astype(jnp.bfloat16)


def attend_kernel(rows, trows, per, q_in, kv_in, out):
    sources, qrows, width = q_in.shape
    count, kvrows, _ = kv_in.shape
    heads = width // HD
    total_q = sources * qrows
    tile = kvrows - 2 * rows
    scale = math.log2(math.e) / math.sqrt(HD)
    pick_k = select_rows(per, tile, 0, trows)
    pick_v = select_rows(per, tile, trows, trows)
    nt = (((1,), (1,)), ((), ()))

    def block(h, start):
        lanes = slice(h * HD, (h + 1) * HD)
        span = pl.ds(start, per)
        k = kv_in[span, :rows, lanes].reshape(per * rows, HD)
        v = kv_in[span, rows : 2 * rows, lanes].reshape(per * rows, HD)
        t = kv_in[span, 2 * rows :, lanes].reshape(per * tile, HD)
        kt = jnp.dot(pick_k, t, preferred_element_type=jnp.float32).astype(jnp.bfloat16)
        vt = jnp.dot(pick_v, t, preferred_element_type=jnp.float32).astype(jnp.bfloat16)
        return k, v, kt, vt

    def scores(q, k):
        return lax.dot_general(q, k, nt, preferred_element_type=jnp.float32)

    def weigh(s, best):
        return jnp.exp2((s - best) * scale).astype(jnp.bfloat16)

    def with_ones(v):
        return jnp.concatenate([v, jnp.ones_like(v)], axis=1)

    for h in range(heads):
        lanes = slice(h * HD, (h + 1) * HD)
        q = q_in[:, :, lanes].reshape(total_q, HD)

        def step(i, state):
            k, v, kt, vt = block(h, i * per)
            s, st = scores(q, k), scores(q, kt)
            best = jnp.maximum(jnp.max(s, axis=1, keepdims=True), jnp.max(st, axis=1, keepdims=True))
            if state is not None:
                best = jnp.maximum(best, state[0])
            new = jnp.dot(weigh(s, best), with_ones(v), preferred_element_type=jnp.float32)
            new += jnp.dot(weigh(st, best), with_ones(vt), preferred_element_type=jnp.float32)
            if state is not None:
                new += state[1] * jnp.exp2((state[0] - best) * scale)
            return best, new

        state = step(0, None)
        if count > per:
            state = lax.fori_loop(1, count // per, step, state)
        summed = state[1]
        o = summed[:, :HD] / summed[:, HD:]
        out[:, :, lanes] = o.reshape(sources, qrows, HD).astype(jnp.bfloat16)


def unpack_kernel(o_in, video_gate, text_gate, video_out, text_out):
    rows, trows = video_out.shape[0], text_out.shape[0]
    groups, _, width = o_in.shape
    for g in range(groups):
        lanes = slice(g * width, (g + 1) * width)
        x = o_in[g, :rows, :].astype(jnp.float32)
        video_out[:, lanes] = (x * video_gate[:, lanes]).astype(jnp.bfloat16)
        x = o_in[g, rows:, :].astype(jnp.float32)[:trows]
        text_out[:, lanes] = (x * text_gate[:, lanes]).astype(jnp.bfloat16)


def pack_halves_kernel(groups, me, video, text, own, *cross):
    rows, trows = video.shape[1], text.shape[1]
    width = own.shape[2]

    def tail(lanes, kinds, total):
        parts = [text[n, :, lanes].astype(jnp.float32) for n in kinds]
        parts.append(jnp.zeros((total - len(kinds) * trows, width), jnp.float32))
        return jnp.concatenate(parts, axis=0).astype(jnp.bfloat16)

    for i, out in enumerate(cross):
        lanes = pl.ds(pl.multiple_of(lax.rem(me[0] + i, groups) * width, HD), width)
        out[:rows, :] = video[1, :, lanes]
        out[rows : 2 * rows, :] = video[2, :, lanes]
        out[2 * rows :, :] = tail(lanes, (1, 2), out.shape[0] - 2 * rows)
    for g in range(groups):
        lanes = slice(g * width, (g + 1) * width)
        for n in range(3):
            own[g, n * rows : (n + 1) * rows, :] = video[n, :, lanes]
        own[g, 3 * rows :, :] = tail(lanes, (0, 1, 2), own.shape[1] - 3 * rows)


def head_queries(own, rows, lanes):
    tile = own.shape[1] - 3 * rows
    q = own[:, :rows, lanes].reshape(-1, HD)
    qt = own[:, 3 * rows :, lanes].reshape(own.shape[0] * tile, HD)
    return jnp.concatenate([q, qt], axis=0)


def dot_nt(a, b):
    return lax.dot_general(a, b, (((1,), (1,)), ((), ())), preferred_element_type=jnp.float32)


def add_keys(q, k, v, kt, vt, state):
    scale = math.log2(math.e) / math.sqrt(HD)
    s, st = dot_nt(q, k), dot_nt(q, kt)
    best = jnp.maximum(jnp.max(s, axis=1, keepdims=True), jnp.max(st, axis=1, keepdims=True))
    if state is not None:
        best = jnp.maximum(best, state[0])
    new = None
    for score, value in ((s, v), (st, vt)):
        weights = jnp.exp2((score - best) * scale).astype(jnp.bfloat16)
        value = jnp.concatenate([value, jnp.ones_like(value)], axis=1)
        term = jnp.dot(weights, value, preferred_element_type=jnp.float32)
        new = term if new is None else new + term
    if state is not None:
        new += state[1] * jnp.exp2((state[0] - best) * scale)
    return best, new


def pick(pick_rows, t):
    return jnp.dot(pick_rows, t, preferred_element_type=jnp.float32).astype(jnp.bfloat16)


def own_kernel(rows, trows, own, state_out):
    groups, total, width = own.shape
    tile = total - 3 * rows
    pick_k = select_rows(groups, tile, trows, trows)
    pick_v = select_rows(groups, tile, 2 * trows, trows)
    for h in range(width // HD):
        lanes = slice(h * HD, (h + 1) * HD)
        q = head_queries(own, rows, lanes)
        k = own[:, rows : 2 * rows, lanes].reshape(groups * rows, HD)
        v = own[:, 2 * rows : 3 * rows, lanes].reshape(groups * rows, HD)
        t = own[:, 3 * rows :, lanes].reshape(groups * tile, HD)
        best, summed = add_keys(q, k, v, pick(pick_k, t), pick(pick_v, t), None)
        state_out[h, :, : 2 * HD] = summed
        state_out[h, :, 2 * HD :] = jnp.broadcast_to(best, (best.shape[0], HD))


def cross_kernel(rows, trows, own, state_in, *rest):
    cross, out = rest[:-1], rest[-1]
    groups, total, width = own.shape
    tile, cross_tile = total - 3 * rows, cross[0].shape[0] - 2 * rows
    pick_k = select_rows(groups, cross_tile, 0, trows)
    pick_v = select_rows(groups, cross_tile, trows, trows)
    for h in range(width // HD):
        lanes = slice(h * HD, (h + 1) * HD)
        q = head_queries(own, rows, lanes)
        k = jnp.concatenate([c[:rows, lanes] for c in cross], axis=0)
        v = jnp.concatenate([c[rows : 2 * rows, lanes] for c in cross], axis=0)
        t = jnp.concatenate([c[2 * rows :, lanes] for c in cross], axis=0)
        state = (state_in[h, :, 2 * HD : 2 * HD + 1], state_in[h, :, : 2 * HD])
        _, summed = add_keys(q, k, v, pick(pick_k, t), pick(pick_v, t), state)
        o = (summed[:, :HD] / summed[:, HD:]).astype(jnp.bfloat16)
        out[:, :rows, lanes] = o[: groups * rows].reshape(groups, rows, HD)
        out[:, rows:, lanes] = o[groups * rows :].reshape(groups, tile, HD)


def two_halves(video_qkv, text_qkv, video_gate, text_gate):
    planes, uly = lax.axis_size("plane"), lax.axis_size("uly")
    groups = planes * uly
    rows, trows = video_qkv.shape[1], text_qkv.shape[1]
    width = HEADS // groups * HD
    own_rows = up(3 * rows + 3 * trows, ROW_TILE)
    cross_rows = up(2 * rows + 2 * trows, ROW_TILE)
    queries = groups * (own_rows - 2 * rows)
    bf16, sds = jnp.bfloat16, jax.ShapeDtypeStruct
    limit = pltpu.CompilerParams(vmem_limit_bytes=40 * 1024 * 1024)
    me = lax.axis_index(("plane", "uly")).astype(jnp.int32).reshape(1)
    own, *cross = pl.pallas_call(
        functools.partial(pack_halves_kernel, groups),
        out_shape=(sds((groups, own_rows, width), bf16),)
        + (sds((cross_rows, width), bf16),) * groups,
        in_specs=[pl.BlockSpec(memory_space=pltpu.SMEM), vspec(), vspec()],
        out_specs=(vspec(),) * (1 + groups),
        name="pack",
    )(me, video_qkv, text_qkv)
    landed = []
    for i, block in enumerate(cross):
        perm = [
            (h * groups + g, (1 - h) * groups + (g + i) % groups)
            for h in range(2)
            for g in range(groups)
        ]
        landed.append(lax.ppermute(block, ("half", "plane", "uly"), perm))
    own = lax.all_to_all(own, ("plane", "uly"), split_axis=0, concat_axis=0, tiled=True)
    heads = width // HD
    flops = 4 * queries * groups * (rows + trows) * width
    cost = pl.CostEstimate(flops=flops, bytes_accessed=4 << 20, transcendentals=0)
    state = pl.pallas_call(
        functools.partial(own_kernel, rows, trows),
        out_shape=sds((heads, queries, 3 * HD), jnp.float32),
        in_specs=[vspec()],
        out_specs=vspec(),
        compiler_params=limit,
        cost_estimate=cost,
        name="own_keys",
    )(own)
    o = pl.pallas_call(
        functools.partial(cross_kernel, rows, trows),
        out_shape=sds((groups, own_rows - 2 * rows, width), bf16),
        in_specs=[vspec()] * (2 + groups),
        out_specs=vspec(),
        compiler_params=limit,
        cost_estimate=cost,
        name="cross_keys",
    )(own, state, *landed)
    back = lax.all_to_all(o, ("plane", "uly"), split_axis=0, concat_axis=0, tiled=True)
    return finish(back, video_gate, text_gate, rows, trows)


def finish(back, video_gate, text_gate, rows, trows):
    return pl.pallas_call(
        unpack_kernel,
        out_shape=(
            jax.ShapeDtypeStruct((rows, HEADS * HD), jnp.bfloat16),
            jax.ShapeDtypeStruct((trows, HEADS * HD), jnp.bfloat16),
        ),
        in_specs=[vspec()] * 3,
        out_specs=(vspec(), vspec()),
        name="unpack",
    )(back, video_gate[None, :], text_gate[None, :])


def on_device(video_qkv, text_qkv, video_gate, text_gate):
    halves, planes, uly = lax.axis_size("half"), lax.axis_size("plane"), lax.axis_size("uly")
    groups = planes * uly
    count = halves * groups
    rows, trows = video_qkv.shape[1], text_qkv.shape[1]
    width = HEADS // groups * HD
    q_rows = up(rows + trows, ROW_TILE)
    kv_rows = up(2 * rows + 2 * trows, ROW_TILE)
    bf16 = jnp.bfloat16
    limit = pltpu.CompilerParams(vmem_limit_bytes=56 * 1024 * 1024)
    q_pack, kv_pack = pl.pallas_call(
        functools.partial(pack_kernel, groups, halves),
        out_shape=(
            jax.ShapeDtypeStruct((groups, q_rows, width), bf16),
            jax.ShapeDtypeStruct((halves, groups, kv_rows, width), bf16),
        ),
        in_specs=[vspec()] * 2,
        out_specs=(vspec(), vspec()),
        name="pack",
    )(video_qkv, text_qkv)
    kv = lax.all_to_all(
        kv_pack.reshape(count, kv_rows, width),
        ("half", "plane", "uly"), split_axis=0, concat_axis=0, tiled=True,
    )
    q = lax.all_to_all(q_pack, ("plane", "uly"), split_axis=0, concat_axis=0, tiled=True)
    per = count
    while per * rows > 1024 and per % 2 == 0:
        per //= 2
    o = pl.pallas_call(
        functools.partial(attend_kernel, rows, trows, per),
        out_shape=jax.ShapeDtypeStruct((groups, q_rows, width), bf16),
        in_specs=[vspec()] * 2,
        out_specs=vspec(),
        compiler_params=limit,
        name="attend",
    )(q, kv)
    back = lax.all_to_all(o, ("plane", "uly"), split_axis=0, concat_axis=0, tiled=True)
    return finish(back, video_gate, text_gate, rows, trows)


def solution(mesh):
    req, blk, uly = (mesh.shape[name] for name in ("req", "blk", "uly"))
    planes = max(p for p in range(1, blk + 1) if blk % p == 0 and HEADS % (p * uly) == 0)
    fine = Mesh(
        mesh.devices.reshape(req, blk // planes, planes, uly), ("req", "half", "plane", "uly")
    )
    every = ("req", "half", "plane", "uly")
    in_specs = (P(None, every, None), P(None, every, None), P("req"), P("req"))
    out_specs = (P(every, None), P(every, None))
    return jax.shard_map(
        two_halves if blk == 2 * planes else on_device, mesh=fine, in_specs=in_specs, out_specs=out_specs, check_vma=False
    )
```

```python
import functools
import math

import jax
import jax.numpy as jnp
from jax import lax
from jax.experimental import pallas as pl
from jax.experimental.pallas import tpu as pltpu
from jax.sharding import Mesh, PartitionSpec as P

HEADS = 24
HD = 128
VMEM = pltpu.VMEM
ROW_TILE = 8


def up(n, m):
    return -(-n // m) * m


def vspec():
    return pl.BlockSpec(memory_space=VMEM)


def pack_kernel(groups, copies, video, text, q_out, kv_out):
    rows, trows = video.shape[1], text.shape[1]
    width = q_out.shape[2]
    q_pad = q_out.shape[1] - rows - trows
    kv_pad = kv_out.shape[2] - 2 * rows - 2 * trows
    for g in range(groups):
        lanes = slice(g * width, (g + 1) * width)
        q_out[g, :rows, :] = video[0, :, lanes]
        parts = [text[0, :, lanes].astype(jnp.float32), jnp.zeros((q_pad, width), jnp.float32)]
        q_out[g, rows:, :] = jnp.concatenate(parts, axis=0).astype(jnp.bfloat16)
        parts = [
            text[1, :, lanes].astype(jnp.float32),
            text[2, :, lanes].astype(jnp.float32),
            jnp.zeros((kv_pad, width), jnp.float32),
        ]
        tail = jnp.concatenate(parts, axis=0).astype(jnp.bfloat16)
        for c in range(copies):
            kv_out[c, g, :rows, :] = video[1, :, lanes]
            kv_out[c, g, rows : 2 * rows, :] = video[2, :, lanes]
            kv_out[c, g, 2 * rows :, :] = tail


def select_rows(count, tile, first, trows):
    i = lax.broadcasted_iota(jnp.int32, (count * trows, count * tile), 0)
    j = lax.broadcasted_iota(jnp.int32, (count * trows, count * tile), 1)
    want = (i // trows) * tile + first + i % trows
    return jnp.where(j == want, 1.0, 0.0).astype(jnp.bfloat16)


def attend_kernel(rows, trows, per, q_in, kv_in, out):
    sources, qrows, width = q_in.shape
    count, kvrows, _ = kv_in.shape
    heads = width // HD
    total_q = sources * qrows
    tile = kvrows - 2 * rows
    scale = math.log2(math.e) / math.sqrt(HD)
    pick_k = select_rows(per, tile, 0, trows)
    pick_v = select_rows(per, tile, trows, trows)
    nt = (((1,), (1,)), ((), ()))

    def block(h, start):
        lanes = slice(h * HD, (h + 1) * HD)
        span = pl.ds(start, per)
        k = kv_in[span, :rows, lanes].reshape(per * rows, HD)
        v = kv_in[span, rows : 2 * rows, lanes].reshape(per * rows, HD)
        t = kv_in[span, 2 * rows :, lanes].reshape(per * tile, HD)
        kt = jnp.dot(pick_k, t, preferred_element_type=jnp.float32).astype(jnp.bfloat16)
        vt = jnp.dot(pick_v, t, preferred_element_type=jnp.float32).astype(jnp.bfloat16)
        return k, v, kt, vt

    def scores(q, k):
        return lax.dot_general(q, k, nt, preferred_element_type=jnp.float32)

    def weigh(s, best):
        return jnp.exp2((s - best) * scale).astype(jnp.bfloat16)

    def with_ones(v):
        return jnp.concatenate([v, jnp.ones_like(v)], axis=1)

    for h in range(heads):
        lanes = slice(h * HD, (h + 1) * HD)
        q = q_in[:, :, lanes].reshape(total_q, HD)

        def step(i, state):
            k, v, kt, vt = block(h, i * per)
            s, st = scores(q, k), scores(q, kt)
            best = jnp.maximum(jnp.max(s, axis=1, keepdims=True), jnp.max(st, axis=1, keepdims=True))
            if state is not None:
                best = jnp.maximum(best, state[0])
            new = jnp.dot(weigh(s, best), with_ones(v), preferred_element_type=jnp.float32)
            new += jnp.dot(weigh(st, best), with_ones(vt), preferred_element_type=jnp.float32)
            if state is not None:
                new += state[1] * jnp.exp2((state[0] - best) * scale)
            return best, new

        state = step(0, None)
        if count > per:
            state = lax.fori_loop(1, count // per, step, state)
        summed = state[1]
        o = summed[:, :HD] / summed[:, HD:]
        out[:, :, lanes] = o.reshape(sources, qrows, HD).astype(jnp.bfloat16)


def unpack_kernel(o_in, video_gate, text_gate, video_out, text_out):
    rows, trows = video_out.shape[0], text_out.shape[0]
    groups, _, width = o_in.shape
    for g in range(groups):
        lanes = slice(g * width, (g + 1) * width)
        x = o_in[g, :rows, :].astype(jnp.float32)
        video_out[:, lanes] = (x * video_gate[:, lanes]).astype(jnp.bfloat16)
        x = o_in[g, rows:, :].astype(jnp.float32)[:trows]
        text_out[:, lanes] = (x * text_gate[:, lanes]).astype(jnp.bfloat16)


def tail_rows(text, lanes, kinds, total):
    trows = text.shape[1]
    parts = [text[n, :, lanes].astype(jnp.float32) for n in kinds]
    parts.append(jnp.zeros((total - len(kinds) * trows, parts[0].shape[1]), jnp.float32))
    return jnp.concatenate(parts, axis=0).astype(jnp.bfloat16)


def pack_cross_kernel(rows, me, video, text, *rest):
    cross, sems = rest[:-1], rest[-1]
    copies = []
    for i, out in enumerate(cross):
        width = out.shape[1]
        lanes = pl.ds(pl.multiple_of((me[0] ^ i) * width, HD), width)
        for n in range(2):
            copy = pltpu.make_async_copy(
                video.at[1 + n, :, lanes], out.at[n * rows : (n + 1) * rows, :], sems.at[i, n]
            )
            copy.start()
            copies.append(copy)
        out[2 * rows :, :] = tail_rows(text, lanes, (1, 2), out.shape[0] - 2 * rows)
    for copy in copies:
        copy.wait()


def pack_own_kernel(rows, video, text, own, sems):
    groups, total, width = own.shape
    copies = []
    for g in range(groups):
        lanes = slice(g * width, (g + 1) * width)
        for n in range(3):
            copy = pltpu.make_async_copy(
                video.at[n, :, lanes], own.at[g, n * rows : (n + 1) * rows, :], sems.at[g, n]
            )
            copy.start()
            copies.append(copy)
        own[g, 3 * rows :, :] = tail_rows(text, lanes, (0, 1, 2), total - 3 * rows)
    for copy in copies:
        copy.wait()


def head_queries(own, rows, lanes):
    tile = own.shape[1] - 3 * rows
    q = own[:, :rows, lanes].reshape(-1, HD)
    qt = own[:, 3 * rows :, lanes].reshape(own.shape[0] * tile, HD)
    return jnp.concatenate([q, qt], axis=0)


def dot_nt(a, b):
    return lax.dot_general(a, b, (((1,), (1,)), ((), ())), preferred_element_type=jnp.float32)


def add_keys(q, k, v, kt, vt, state):
    scale = math.log2(math.e) / math.sqrt(HD)
    s, st = dot_nt(q, k), dot_nt(q, kt)
    best = jnp.maximum(jnp.max(s, axis=1, keepdims=True), jnp.max(st, axis=1, keepdims=True))
    if state is not None:
        best = jnp.maximum(best, state[0])
    new = None
    for score, value in ((s, v), (st, vt)):
        weights = jnp.exp2((score - best) * scale).astype(jnp.bfloat16)
        value = jnp.concatenate([value, jnp.ones_like(value)], axis=1)
        term = jnp.dot(weights, value, preferred_element_type=jnp.float32)
        new = term if new is None else new + term
    if state is not None:
        new += state[1] * jnp.exp2((state[0] - best) * scale)
    return best, new


def pick(pick_rows, t):
    return jnp.dot(pick_rows, t, preferred_element_type=jnp.float32).astype(jnp.bfloat16)


def own_kernel(rows, trows, own, state_out):
    groups, total, width = own.shape
    tile = total - 3 * rows
    pick_k = select_rows(groups, tile, trows, trows)
    pick_v = select_rows(groups, tile, 2 * trows, trows)
    for h in range(width // HD):
        lanes = slice(h * HD, (h + 1) * HD)
        q = head_queries(own, rows, lanes)
        k = own[:, rows : 2 * rows, lanes].reshape(groups * rows, HD)
        v = own[:, 2 * rows : 3 * rows, lanes].reshape(groups * rows, HD)
        t = own[:, 3 * rows :, lanes].reshape(groups * tile, HD)
        best, summed = add_keys(q, k, v, pick(pick_k, t), pick(pick_v, t), None)
        state_out[h, :, : 2 * HD] = summed
        state_out[h, :, 2 * HD :] = jnp.broadcast_to(best, (best.shape[0], HD))


def cross_kernel(rows, trows, own, state_in, *rest):
    cross, out = rest[:-1], rest[-1]
    groups, total, width = own.shape
    tile, cross_tile = total - 3 * rows, cross[0].shape[0] - 2 * rows
    pick_k = select_rows(groups, cross_tile, 0, trows)
    pick_v = select_rows(groups, cross_tile, trows, trows)
    for h in range(width // HD):
        lanes = slice(h * HD, (h + 1) * HD)
        q = head_queries(own, rows, lanes)
        k = jnp.concatenate([c[:rows, lanes] for c in cross], axis=0)
        v = jnp.concatenate([c[rows : 2 * rows, lanes] for c in cross], axis=0)
        t = jnp.concatenate([c[2 * rows :, lanes] for c in cross], axis=0)
        state = (state_in[h, :, 2 * HD : 2 * HD + 1], state_in[h, :, : 2 * HD])
        _, summed = add_keys(q, k, v, pick(pick_k, t), pick(pick_v, t), state)
        o = (summed[:, :HD] / summed[:, HD:]).astype(jnp.bfloat16)
        out[:, :rows, lanes] = o[: groups * rows].reshape(groups, rows, HD)
        out[:, rows:, lanes] = o[groups * rows :].reshape(groups, tile, HD)


def two_halves(video_qkv, text_qkv, video_gate, text_gate):
    planes, uly = lax.axis_size("plane"), lax.axis_size("uly")
    groups = planes * uly
    rows, trows = video_qkv.shape[1], text_qkv.shape[1]
    width = HEADS // groups * HD
    own_rows = up(3 * rows + 3 * trows, ROW_TILE)
    cross_rows = up(2 * rows + 2 * trows, ROW_TILE)
    queries = groups * (own_rows - 2 * rows)
    bf16, sds = jnp.bfloat16, jax.ShapeDtypeStruct
    limit = pltpu.CompilerParams(vmem_limit_bytes=40 * 1024 * 1024)
    me = lax.axis_index(("plane", "uly")).astype(jnp.int32).reshape(1)
    smem, hbm = pl.BlockSpec(memory_space=pltpu.SMEM), pl.BlockSpec(memory_space=pl.ANY)
    small = pltpu.CompilerParams(vmem_limit_bytes=8 * 1024 * 1024)
    cross = pl.pallas_call(
        functools.partial(pack_cross_kernel, rows),
        out_shape=(sds((cross_rows, width), bf16),) * groups,
        in_specs=[smem, hbm, vspec()],
        out_specs=(vspec(),) * groups,
        scratch_shapes=[pltpu.SemaphoreType.DMA((groups, 2))],
        compiler_params=small,
        name="pack_cross",
    )(me, video_qkv, text_qkv)
    own = pl.pallas_call(
        functools.partial(pack_own_kernel, rows),
        out_shape=sds((groups, own_rows, width), bf16),
        in_specs=[hbm, vspec()],
        out_specs=vspec(),
        scratch_shapes=[pltpu.SemaphoreType.DMA((groups, 3))],
        compiler_params=small,
        name="pack_own",
    )(video_qkv, text_qkv)
    landed = []
    for i, block in enumerate(cross):
        perm = [
            (h * groups + g, (1 - h) * groups + (g ^ i))
            for h in range(2)
            for g in range(groups)
        ]
        landed.append(lax.ppermute(block, ("half", "plane", "uly"), perm))
    own = lax.all_to_all(own, ("plane", "uly"), split_axis=0, concat_axis=0, tiled=True)
    heads = width // HD
    flops = 4 * queries * groups * (rows + trows) * width
    cost = pl.CostEstimate(flops=flops, bytes_accessed=4 << 20, transcendentals=0)
    state = pl.pallas_call(
        functools.partial(own_kernel, rows, trows),
        out_shape=sds((heads, queries, 3 * HD), jnp.float32),
        in_specs=[vspec()],
        out_specs=vspec(),
        compiler_params=limit,
        cost_estimate=cost,
        name="own_keys",
    )(own)
    o = pl.pallas_call(
        functools.partial(cross_kernel, rows, trows),
        out_shape=sds((groups, own_rows - 2 * rows, width), bf16),
        in_specs=[vspec()] * (2 + groups),
        out_specs=vspec(),
        compiler_params=limit,
        cost_estimate=cost,
        name="cross_keys",
    )(own, state, *landed)
    back = lax.all_to_all(o, ("plane", "uly"), split_axis=0, concat_axis=0, tiled=True)
    return finish(back, video_gate, text_gate, rows, trows)


def finish(back, video_gate, text_gate, rows, trows):
    return pl.pallas_call(
        unpack_kernel,
        out_shape=(
            jax.ShapeDtypeStruct((rows, HEADS * HD), jnp.bfloat16),
            jax.ShapeDtypeStruct((trows, HEADS * HD), jnp.bfloat16),
        ),
        in_specs=[vspec()] * 3,
        out_specs=(vspec(), vspec()),
        compiler_params=pltpu.CompilerParams(vmem_limit_bytes=8 * 1024 * 1024),
        name="unpack",
    )(back, video_gate[None, :], text_gate[None, :])


def on_device(video_qkv, text_qkv, video_gate, text_gate):
    halves, planes, uly = lax.axis_size("half"), lax.axis_size("plane"), lax.axis_size("uly")
    groups = planes * uly
    count = halves * groups
    rows, trows = video_qkv.shape[1], text_qkv.shape[1]
    width = HEADS // groups * HD
    q_rows = up(rows + trows, ROW_TILE)
    kv_rows = up(2 * rows + 2 * trows, ROW_TILE)
    bf16 = jnp.bfloat16
    limit = pltpu.CompilerParams(vmem_limit_bytes=56 * 1024 * 1024)
    q_pack, kv_pack = pl.pallas_call(
        functools.partial(pack_kernel, groups, halves),
        out_shape=(
            jax.ShapeDtypeStruct((groups, q_rows, width), bf16),
            jax.ShapeDtypeStruct((halves, groups, kv_rows, width), bf16),
        ),
        in_specs=[vspec()] * 2,
        out_specs=(vspec(), vspec()),
        name="pack",
    )(video_qkv, text_qkv)
    kv = lax.all_to_all(
        kv_pack.reshape(count, kv_rows, width),
        ("half", "plane", "uly"), split_axis=0, concat_axis=0, tiled=True,
    )
    q = lax.all_to_all(q_pack, ("plane", "uly"), split_axis=0, concat_axis=0, tiled=True)
    per = count
    while per * rows > 1024 and per % 2 == 0:
        per //= 2
    o = pl.pallas_call(
        functools.partial(attend_kernel, rows, trows, per),
        out_shape=jax.ShapeDtypeStruct((groups, q_rows, width), bf16),
        in_specs=[vspec()] * 2,
        out_specs=vspec(),
        compiler_params=limit,
        name="attend",
    )(q, kv)
    back = lax.all_to_all(o, ("plane", "uly"), split_axis=0, concat_axis=0, tiled=True)
    return finish(back, video_gate, text_gate, rows, trows)


def solution(mesh):
    req, blk, uly = (mesh.shape[name] for name in ("req", "blk", "uly"))
    planes = max(p for p in range(1, blk + 1) if blk % p == 0 and HEADS % (p * uly) == 0)
    fine = Mesh(
        mesh.devices.reshape(req, blk // planes, planes, uly), ("req", "half", "plane", "uly")
    )
    every = ("req", "half", "plane", "uly")
    in_specs = (P(None, every, None), P(None, every, None), P("req"), P("req"))
    out_specs = (P(every, None), P(every, None))
    split = blk == 2 * planes and (planes * uly) & (planes * uly - 1) == 0
    return jax.shard_map(
        two_halves if split else on_device,
        mesh=fine, in_specs=in_specs, out_specs=out_specs, check_vma=False,
    )
```
